128 devices in a mesh: dp: 4 (over z_hi, core), seq: 32 (over y, x, z_lo).
Axes of the slice: x: 4, y: 4, z: 4 (z_hi: 2, z_lo: 2; z = z_hi * 2 + z_lo), core: 2. Of those that a mesh axis runs over, the one named last changes fastest.
Arguments:
- tile_embed: bfloat16 [4, 4096, 768], P('dp', 'seq'), may hold values from -6 to 6
- qkv_saved: bfloat16 [4, 4096, 1152], P('dp', 'seq'), may hold values from -8 to 8
- out_cotangent: bfloat16 [4, 4096, 768], P('dp', 'seq'), may hold values from -6 to 6
- qkv_weight: bfloat16 [768, 1152], replicated, may hold values from -0.21875 to 0.21875
- out_weight: bfloat16 [384, 768], replicated, may hold values from -0.3125 to 0.3125
- seg_length: int32 [8], replicated, may hold values from 128 to 4096, as said below
- dilation: int32 [8], replicated, may hold values from 1 to 4
- owner_map: int32 [4, 4096, 1], P('dp', 'seq'), may hold values from 0 to 31; in each aligned block of 128 rows (0 to 127, 128 to 255, ..., all dimensions but the last counted through in order) at most 8 rows name the same one
- tile_hidden: bfloat16 [4, 8192, 1536], P('dp', 'seq'), may hold values from -6 to 6
- tile_output: bfloat16 [4, 8192, 1536], P('dp', 'seq'), may hold values from -6 to 6
- embed_weight: bfloat16 [1536, 768], replicated, may hold values from -0.15625 to 0.15625
- proj_weight: bfloat16 [1536, 1536], replicated, may hold values from -0.15625 to 0.15625
Outputs:
- hidden_grad: bfloat16 [4, 8192, 1536], P('dp', 'seq')
- proj_weight_grad: float32 [1536, 1536], P(('dp', 'seq'))
- embed_weight_grad: float32 [1536, 768], P(('dp', 'seq'))
- qkv_weight_grad: float32 [768, 1152], P(('dp', 'seq'))
- out_weight_grad: float32 [384, 768], P(('dp', 'seq'))
The draws below stay inside these ranges and needn't reach their ends.
Inputs may be any that keep to these rules, and one draw needn't show every extreme that they name: `seg_length`: each is 128 times a power of two; some head has 4096. `owner_map`: among the 128 positions of one device, no device index is named more than 8 times.
All inputs are finite; a program needn't handle non-finite values.
Results may differ from the reference program's by a relative error of at most 0.015.
Values may be sent and summed in bfloat16 or wider, within the bound.
No kernel may reach another device: no remote copies, remote signals or barrier semaphores. Data moves between devices by JAX's collectives and lax.ppermute only.
A program may use at most 128 MiB of HBM per device.

```python
import math
import jax
import jax.numpy as jnp
import numpy as np
from jax import lax

D_SLIDE = 768
HEADS = 8
HEAD_DIM = 48
D_TILE = 1536
TOK_DEV = 128
LENGTH = 4096
CAP = 8
SLOTS = 256
ROWS_ALL = 8192
N_DP = 4
N_SEQ = 32


def draw_qkv_saved(key, part):
    width = HEADS * HEAD_DIM
    shape = (N_DP, LENGTH, 3 * width)
    values_drawn = jnp.clip(jax.random.normal(key, shape, jnp.float32), -8.0, 8.0)
    return values_drawn.astype(jnp.bfloat16)


def draw_seg_length(key, part):
    levels = N_SEQ.bit_length()
    powers = jax.random.randint(jax.random.fold_in(key, 3), (HEADS,), 0, levels)
    powers = powers.at[0].set(levels - 1)
    powers = jax.random.permutation(jax.random.fold_in(key, 5), powers)
    return (jnp.left_shift(jnp.ones((HEADS,), jnp.int32), powers.astype(jnp.int32)) * TOK_DEV).astype(jnp.int32)


def set_ends(drawn, stream_key, smallest, largest):
    shape = drawn.shape
    spot = [jax.random.randint(jax.random.fold_in(stream_key, axis), (), 0, shape[axis]) for axis in range(len(shape))]
    drawn = drawn.at[tuple(spot)].set(smallest)
    longest = shape.index(max(shape))
    spot[longest] = (spot[longest] + 1) % shape[longest]
    return drawn.at[tuple(spot)].set(largest)


def shard_levels(key, extent, cuts, least, top_value):
    factor_of, own = 1.0, jax.random.fold_in(key, 6)
    for dim, parts in cuts:
        heights = jnp.exp(jax.random.uniform(jax.random.fold_in(own, dim), (parts,), jnp.float32, least / len(cuts), top_value / len(cuts)))
        factor_of = factor_of * jnp.repeat(heights, extent[dim] // parts).reshape([-1 if axis == dim else 1 for axis in range(len(extent))])
    return factor_of


def routed_block(key, own, number, rows, amount, top, limit, slope):
    ranking = jax.random.permutation(key, amount)
    crowded, common = load_shares(amount, rows * top, limit, slope, True), load_shares(amount, rows * top, limit, slope, False)
    places = jnp.arange(amount)

    def named(sizes, offset_by):
        used = int((sizes > 0).sum())
        fixed = max(1, used // 4)
        passed = fixed + (places - fixed + offset_by * (used - fixed)) % max(1, amount - fixed)
        return jnp.zeros((amount,), jnp.int32).at[ranking[jnp.where(places < fixed, places, passed)]].set(jnp.asarray(sizes, jnp.int32))

    sizes = jnp.where(number % 4 == 0, named(crowded, number // 4), named(common, number - number // 4 - 1))
    mixed = jax.random.permutation(jax.random.fold_in(own, 3), amount)
    donor, sink = mixed[0:amount // 2 * 2:2], mixed[1:amount // 2 * 2:2]
    room = jnp.minimum(sizes[donor] - 1, limit - sizes[sink]) // 2
    room = jnp.where((donor == ranking[0]) | (sink == ranking[0]) | (sizes[sink] == 0), 0, jnp.maximum(room, 0))
    passed = jax.random.randint(jax.random.fold_in(own, 4), (amount // 2,), 0, 1 << 20) % (room + 1)
    sizes = sizes.at[donor].add(-passed).at[sink].add(passed)
    labels = jnp.searchsorted(jnp.cumsum(sizes), jnp.arange(rows * top), side="right").astype(jnp.int32)
    grid = labels.reshape(top, rows).T
    grid = grid[jax.random.permutation(jax.random.fold_in(own, 1), rows)]
    offset_by = jax.random.randint(jax.random.fold_in(own, 2), (rows, 1), 0, top)
    return jnp.take_along_axis(grid, (jnp.arange(top)[None, :] + offset_by) % top, axis=1)


def load_shares(number_of, total, most, skew, full):
    portions = [(1 << 20) // math.isqrt(standing ** skew) + 1 for standing in range(1, number_of + 1)]
    largest = most if full else min(most, max(-(-total // number_of), total * portions[0] // sum(portions)))
    least = 1 if total - largest >= number_of - 1 else 0
    holding, rest = [largest] + [least] * (number_of - 1), total - largest - least * (number_of - 1)
    while rest > 0:
        free = [i for i in range(1, number_of) if holding[i] < largest] or [i for i in range(1, number_of) if holding[i] < most]
        pool, budget = sum([portions[i] for i in free]), rest
        for i in free:
            addition = min(most - holding[i], max(1, budget * portions[i] // pool), rest)
            holding[i] = holding[i] + addition
            rest = rest - addition
    return np.array(holding)


def noise(stream_key, dims, deviation, bound, shards=(), kind=jnp.bfloat16):
    gain = shard_levels(stream_key, dims, shards, -0.22, 0.18) if shards else 1.0
    drawn = jax.random.normal(stream_key, dims, jnp.float32) * deviation * gain
    return jnp.minimum(jnp.maximum(drawn, -bound), bound).astype(kind)


def setup_inputs(seed: int = 0) -> dict:
    key_list = jax.random.split(jax.random.key(seed), 13)
    tile_embed = noise(key_list[0], (N_DP, LENGTH, D_SLIDE), 1.0, 6.0, ((0, 4), (1, 32)))
    qkv_saved = draw_qkv_saved(jax.random.fold_in(key_list[12], 71), 0)
    out_cotangent = noise(key_list[2], (N_DP, LENGTH, D_SLIDE), 1.0, 6.0, ((0, 4), (1, 32)))
    qkv_weight = noise(key_list[3], (D_SLIDE, 3 * HEADS * HEAD_DIM), D_SLIDE ** -0.5, 0.21875)
    out_weight = noise(key_list[4], (HEADS * HEAD_DIM, D_SLIDE), (HEADS * HEAD_DIM) ** -0.5, 0.3125)
    seg_length = draw_seg_length(jax.random.fold_in(key_list[12], 71), 0)
    dilation = set_ends(jax.random.randint(key_list[6], (HEADS,), 1, 5), jax.random.fold_in(key_list[6], 1), 1, 4).astype(jnp.int32)
    owner_map_keys = jax.random.split(jax.random.fold_in(key_list[7], 1), N_DP * LENGTH // TOK_DEV)
    owner_map_turns = jax.random.permutation(jax.random.fold_in(key_list[7], 3), N_DP * LENGTH // TOK_DEV)
    owner_map = jax.vmap(lambda own, number: routed_block(jax.random.fold_in(key_list[7], 2), own, number, TOK_DEV, N_SEQ, 1, CAP, 2))(owner_map_keys, owner_map_turns).reshape((N_DP, LENGTH, 1))
    tile_hidden = noise(key_list[8], (N_DP, ROWS_ALL, D_TILE), 1.0, 6.0, ((0, 4), (1, 32)))
    tile_output = noise(key_list[9], (N_DP, ROWS_ALL, D_TILE), 1.0, 6.0, ((0, 4), (1, 32)))
    embed_weight = noise(key_list[10], (D_TILE, D_SLIDE), D_TILE ** -0.5, 0.15625)
    proj_weight = noise(key_list[11], (D_TILE, D_TILE), D_TILE ** -0.5, 0.15625)
    return dict(tile_embed=tile_embed, qkv_saved=qkv_saved, out_cotangent=out_cotangent, qkv_weight=qkv_weight, out_weight=out_weight, seg_length=seg_length, dilation=dilation, owner_map=owner_map, tile_hidden=tile_hidden, tile_output=tile_output, embed_weight=embed_weight, proj_weight=proj_weight)


def head_math(queries, keys_all, values_all, grads_out, span, stride, query_pos, key_pos, scaling):
    allowed = (query_pos[:, None] // span == key_pos[None, :] // span) & ((key_pos[None, :] - query_pos[:, None]) % stride == 0)
    scores = jnp.einsum("qd,kd->qk", queries, keys_all) * scaling
    scores = jnp.where(allowed, scores, -1e30)
    shifted = jnp.exp(scores - jnp.max(scores, axis=1, keepdims=True))
    probs_full = shifted / jnp.sum(shifted, axis=1, keepdims=True)
    probs_half = probs_full.astype(jnp.bfloat16).astype(jnp.float32)
    head_out = jnp.einsum("qk,kd->qd", probs_half, values_all)
    prob_grad = jnp.einsum("qd,kd->qk", grads_out, values_all)
    row_delta = jnp.sum(probs_full * prob_grad, axis=1, keepdims=True)
    score_grad = (probs_full * (prob_grad - row_delta) * scaling).astype(jnp.bfloat16).astype(jnp.float32)
    query_grad = jnp.einsum("qk,kd->qd", score_grad, keys_all)
    key_grad = jnp.einsum("qk,qd->kd", score_grad, queries)
    value_grad = jnp.einsum("qk,qd->kd", probs_half, grads_out)
    return head_out, query_grad, key_grad, value_grad


def split_heads(block, head_count, head_width):
    return block.reshape(block.shape[0], head_count, head_width).transpose(1, 0, 2)


def merge_heads(block):
    return block.transpose(1, 0, 2).reshape(block.shape[1], block.shape[0] * block.shape[2])


def slide_pass(embed_rows, saved, cotangent, qkv_weight, out_weight, seg_length, dilation):
    head_count = seg_length.shape[0]
    heads_width = out_weight.shape[0]
    head_width = heads_width // head_count
    length = saved.shape[0]
    scaling = head_width ** -0.5
    grads_out = jnp.dot(cotangent, out_weight.T, preferred_element_type=jnp.float32).astype(jnp.bfloat16)
    queries = split_heads(saved[:, :heads_width].astype(jnp.float32), head_count, head_width)
    keys_all = split_heads(saved[:, heads_width:2 * heads_width].astype(jnp.float32), head_count, head_width)
    values_all = split_heads(saved[:, 2 * heads_width:].astype(jnp.float32), head_count, head_width)
    grads_heads = split_heads(grads_out.astype(jnp.float32), head_count, head_width)
    key_pos = jnp.arange(length, dtype=jnp.int32)

    def block_step(carry, block_index):
        first_row = (block_index * TOK_DEV).astype(jnp.int32)
        query_pos = first_row + jnp.arange(TOK_DEV, dtype=jnp.int32)
        query_rows = lax.dynamic_slice_in_dim(queries, first_row, TOK_DEV, 1)
        grad_rows = lax.dynamic_slice_in_dim(grads_heads, first_row, TOK_DEV, 1)
        head_out, query_grad, key_grad, value_grad = jax.vmap(
            lambda qh, kh, vh, gh, span, stride: head_math(qh, kh, vh, gh, span, stride, query_pos, key_pos, scaling)
        )(query_rows, keys_all, values_all, grad_rows, seg_length, dilation)
        term = jnp.concatenate([merge_heads(key_grad), merge_heads(value_grad)], axis=1)
        rounded = lax.optimization_barrier(term.astype(jnp.bfloat16))
        return carry + rounded.astype(jnp.float32), (merge_heads(head_out), merge_heads(query_grad))

    start = jnp.zeros((length, 2 * heads_width), jnp.float32)
    summed, (outs, qgrads) = lax.scan(block_step, start, jnp.arange(N_SEQ, dtype=jnp.int32))
    attention = outs.reshape(length, heads_width).astype(jnp.bfloat16)
    query_grad = qgrads.reshape(length, heads_width)
    qkv_grad = jnp.concatenate([query_grad, summed], axis=1).astype(jnp.bfloat16)
    embed_grad = (cotangent.astype(jnp.float32) + jnp.dot(qkv_grad, qkv_weight.T, preferred_element_type=jnp.float32)).astype(jnp.bfloat16)
    qkv_term = jnp.dot(embed_rows.T, qkv_grad, preferred_element_type=jnp.float32)
    out_term = jnp.dot(attention.T, cotangent, preferred_element_type=jnp.float32)
    return embed_grad, qkv_term, out_term


def reference(tile_embed, qkv_saved, out_cotangent, qkv_weight, out_weight, seg_length, dilation, owner_map, tile_hidden, tile_output, embed_weight, proj_weight):
    length = qkv_saved.shape[1]
    hidden_list = []
    qkv_sum = jnp.zeros(qkv_weight.shape, jnp.float32)
    out_sum = jnp.zeros(out_weight.shape, jnp.float32)
    embed_sum = jnp.zeros(embed_weight.shape, jnp.float32)
    proj_sum = jnp.zeros(proj_weight.shape, jnp.float32)
    for slide in range(N_DP):
        embed_grad, qkv_term, out_term = slide_pass(tile_embed[slide], qkv_saved[slide], out_cotangent[slide], qkv_weight, out_weight, seg_length, dilation)
        qkv_sum = qkv_sum + qkv_term
        out_sum = out_sum + out_term
        destination = owner_map[slide, :, 0].astype(jnp.int32)
        blocked = destination.reshape(N_SEQ, TOK_DEV)
        onehot = (blocked[:, :, None] == jnp.arange(N_SEQ, dtype=jnp.int32)[None, None, :]).astype(jnp.int32)
        before = jnp.cumsum(onehot, axis=1) - onehot
        slot_rank = jnp.sum(before * onehot, axis=2).reshape(length)
        source = jnp.arange(length, dtype=jnp.int32) // TOK_DEV
        row_index = (destination * SLOTS + source * CAP + slot_rank).astype(jnp.int32)
        incoming = jnp.zeros((ROWS_ALL, embed_grad.shape[1]), jnp.bfloat16).at[row_index].set(embed_grad)
        tile_grad = jnp.dot(incoming, embed_weight.T, preferred_element_type=jnp.float32)
        hidden_list.append(jnp.dot(tile_grad.astype(jnp.bfloat16), proj_weight.T, preferred_element_type=jnp.float32).astype(jnp.bfloat16))
        embed_sum = embed_sum + jnp.dot(tile_output[slide].T, incoming, preferred_element_type=jnp.float32)
        proj_sum = proj_sum + jnp.dot(tile_hidden[slide].astype(jnp.float32).T, tile_grad, precision=lax.Precision.HIGHEST)
    return jnp.stack(hidden_list), proj_sum, embed_sum, qkv_sum, out_sum
```

```python
from functools import partial

import jax
import jax.numpy as jnp
from jax import lax
from jax.experimental import pallas as pl
from jax.experimental.pallas import tpu as pltpu
from jax.sharding import Mesh, PartitionSpec as P

F32 = jnp.float32
BF16 = jnp.bfloat16
DP = ("zh", "co")
SEQ = ("y", "x", "zl")
GRP = ("x", "zl")
ALL = DP + SEQ
QB = 256
KC = 512
LOG2E = 1.4426950408889634


def exchange(x, axes):
    return lax.all_to_all(x, axes, 0, 0, tiled=True)


def sent_to_all(x, axes):
    n = lax.axis_size(axes)
    return exchange(jnp.broadcast_to(x[None], (n, *x.shape)), axes)


def attention_kernel(
    par, kv, qd, dkv, qo, kmat, vmat, kt, vt, code, score, prob, dk, dv, *, hd, tok, nkb, scaling
):
    step = pl.program_id(0)
    length = nkb * tok
    off = par[0]
    inv_len, dil, inv_dil = par[1], par[2], par[3]

    def code_of(pos):
        seg = jnp.floor((pos + 0.5) * inv_len)
        res = pos - dil * jnp.floor((pos + 0.5) * inv_dil)
        return seg * 8.0 + res

    @pl.when(step == 0)
    def _():
        for b in range(nkb):
            kb = kv[b, :hd, :]
            vb = kv[b, hd:, :]
            kt[:, b * tok : (b + 1) * tok] = kb
            vt[:, b * tok : (b + 1) * tok] = vb
            kmat[b * tok : (b + 1) * tok, :] = kb.astype(F32).T.astype(BF16)
            vmat[b * tok : (b + 1) * tok, :] = vb.astype(F32).T.astype(BF16)
            pos = lax.broadcasted_iota(jnp.int32, (tok, 128), 0).astype(F32) + float(b * tok)
            code[b * tok : (b + 1) * tok, :] = code_of(pos)
        dk[...] = jnp.zeros_like(dk)
        dv[...] = jnp.zeros_like(dv)

    nb = QB // tok
    qt = jnp.concatenate([qd[b, :hd, :] for b in range(nb)], axis=1)
    dot_ = jnp.concatenate([qd[b, hd:, :] for b in range(nb)], axis=1).astype(F32)
    qpos = lax.broadcasted_iota(jnp.int32, (8, QB), 1).astype(F32) + off + (step * QB).astype(F32)
    qcode = code_of(qpos)[0:1, :]

    mx = jnp.full((8, QB), -3e38, F32)
    for c in range(length // KC):
        rows = slice(c * KC, (c + 1) * KC)
        s = jnp.dot(kmat[rows, :], qt, preferred_element_type=F32)
        ck = code[rows, :]
        s = jnp.where(jnp.concatenate([ck] * (QB // 128), axis=1) == qcode, s, -1e30)
        score[rows, :] = s
        mx = jnp.maximum(mx, jnp.max(s.reshape(KC // 8, 8, QB), axis=0))
    top = jnp.max(mx, axis=0, keepdims=True)

    tot = jnp.zeros((8, QB), F32)
    ot = jnp.zeros((hd, QB), F32)
    for c in range(length // KC):
        rows = slice(c * KC, (c + 1) * KC)
        p = jnp.exp2((score[rows, :] - top) * (scaling * LOG2E))
        tot = tot + jnp.sum(p.reshape(KC // 8, 8, QB), axis=0)
        ph = p.astype(BF16)
        prob[rows, :] = ph
        ot = ot + jnp.dot(vt[:, rows], ph, preferred_element_type=F32)
    inv = 1.0 / jnp.sum(tot, axis=0, keepdims=True)
    ot = ot * inv
    dn = dot_ * inv
    dnh = dn.astype(BF16)
    delta = jnp.sum(dnh.astype(F32) * ot, axis=0, keepdims=True)
    dmat = dn.T.astype(BF16)
    qmat = qt.astype(F32).T.astype(BF16)

    dqt = jnp.zeros((hd, QB), F32)
    for c in range(length // KC):
        rows = slice(c * KC, (c + 1) * KC)
        ph = prob[rows, :]
        dp = jnp.dot(vmat[rows, :], dnh, preferred_element_type=F32)
        ds = (ph.astype(F32) * (dp - delta)).astype(BF16)
        dv[rows, :] += jnp.dot(ph, dmat, preferred_element_type=F32)
        dk[rows, :] += jnp.dot(ds, qmat, preferred_element_type=F32)
        dqt = dqt + jnp.dot(kt[:, rows], ds, preferred_element_type=F32)

    for b in range(nb):
        cols = slice(b * tok, (b + 1) * tok)
        qo[b, :hd, :] = (dqt[:, cols] * scaling).astype(BF16)
        qo[b, hd:, :] = ot[:, cols].astype(BF16)

    @pl.when(step == pl.num_programs(0) - 1)
    def _():
        for b in range(nkb):
            rows = slice(b * tok, (b + 1) * tok)
            dkv[b, :hd, :] = (dk[rows, :].T * scaling).astype(BF16)
            dkv[b, hd:, :] = dv[rows, :].T.astype(BF16)


def attention_grads(par, kv, qd, scaling):
    nkb, two, tok = kv.shape
    hd = two // 2
    nqb = qd.shape[0]
    length = nkb * tok
    steps = nqb * tok // QB
    nb = QB // tok
    return pl.pallas_call(
        partial(attention_kernel, hd=hd, tok=tok, nkb=nkb, scaling=scaling),
        grid=(steps,),
        out_shape=(
            jax.ShapeDtypeStruct((nkb, two, tok), BF16),
            jax.ShapeDtypeStruct((nqb, two, tok), BF16),
        ),
        in_specs=[
            pl.BlockSpec(memory_space=pltpu.SMEM),
            pl.BlockSpec((nkb, two, tok), lambda i: (0, 0, 0)),
            pl.BlockSpec((nb, two, tok), lambda i: (i, 0, 0)),
        ],
        out_specs=(
            pl.BlockSpec((nkb, two, tok), lambda i: (0, 0, 0)),
            pl.BlockSpec((nb, two, tok), lambda i: (i, 0, 0)),
        ),
        scratch_shapes=[
            pltpu.VMEM((length, hd), BF16),
            pltpu.VMEM((length, hd), BF16),
            pltpu.VMEM((hd, length), BF16),
            pltpu.VMEM((hd, length), BF16),
            pltpu.VMEM((length, 128), F32),
            pltpu.VMEM((length, QB), F32),
            pltpu.VMEM((length, QB), BF16),
            pltpu.VMEM((length, hd), F32),
            pltpu.VMEM((length, hd), F32),
        ],
        compiler_params=pltpu.CompilerParams(dimension_semantics=("arbitrary",)),
        cost_estimate=pl.CostEstimate(
            flops=30_000_000_000, bytes_accessed=4_000_000, transcendentals=length * nqb * tok
        ),
        name="attention_grads",
    )(par, kv, qd)


def local(
    tile_embed,
    qkv_saved,
    out_cotangent,
    qkv_weight,
    out_weight,
    seg_length,
    dilation,
    owner_map,
    tile_hidden,
    tile_output,
    embed_weight,
    proj_weight,
):
    heads = seg_length.shape[0]
    width = out_weight.shape[0]
    hd = width // heads
    tok = qkv_saved.shape[1]
    d_slide = tile_embed.shape[2]
    n_seq = lax.axis_size(SEQ)
    n_y = lax.axis_size("y")
    n_grp = lax.axis_size(GRP)
    n_dp = lax.axis_size(DP)
    n_dev = n_dp * n_seq
    scaling = hd ** (-0.5)
    cot = out_cotangent[0]
    head = lax.axis_index(GRP)
    core = lax.axis_index("co")

    saved_t = qkv_saved[0].T.reshape(3, heads, hd, tok)
    grads_t = jnp.einsum("cd,td->ct", out_weight, cot, preferred_element_type=F32)
    grads_t = grads_t.astype(BF16).reshape(heads, hd, tok)
    outgoing = jnp.concatenate([saved_t[0], grads_t, saved_t[1], saved_t[2]], axis=1)
    mine = exchange(outgoing, GRP)
    qd = mine[:, : 2 * hd]
    kv = sent_to_all(mine[:, 2 * hd :], "y").reshape(n_seq, 2 * hd, tok)

    seg = seg_length[head].astype(F32)
    dil = dilation[head].astype(F32)
    off = (lax.axis_index("y") * n_grp * tok).astype(F32)
    par = jnp.stack([off, 1.0 / seg, dil, 1.0 / dil])
    dkv, qo = attention_grads(par, kv, qd, scaling)

    embed_all = sent_to_all(tile_embed[0], GRP).reshape(n_grp * tok, d_slide)
    pick = jnp.where(core == 0, tile_hidden[0], tile_output[0])
    keep = jnp.where(core == 0, tile_output[0], tile_hidden[0])
    other = lax.ppermute(pick, "co", [(0, 1), (1, 0)])

    terms = exchange(dkv.reshape(n_y, n_grp, 2 * hd, tok), "y")
    dkv_sum = jnp.sum(terms.astype(F32), axis=0).astype(BF16)
    back = jnp.concatenate([qo, dkv_sum], axis=1)
    got = exchange(back, GRP)

    grad_t = jnp.concatenate([qo[:, :hd], dkv_sum], axis=1).transpose(1, 0, 2)
    grad_t = grad_t.reshape(3 * hd, n_grp * tok)
    qkv_term = jnp.einsum("td,ct->dc", embed_all, grad_t, preferred_element_type=F32)
    qkv_term = qkv_term.astype(BF16).reshape(n_dp * n_y, -1, 3 * hd)
    qkv_part = jnp.sum(exchange(qkv_term, DP + ("y",)).astype(F32), axis=0)
    qkv_part = exchange(qkv_part.reshape(n_grp, -1, 3 * hd), GRP)
    rows = qkv_part.shape[1]
    qkv_sum = qkv_part.reshape(heads, rows, 3, hd).transpose(1, 2, 0, 3).reshape(rows, 3 * width)

    got = got.reshape(heads, 4, hd, tok)
    attention_t = got[:, 1].reshape(width, tok)
    qkv_grad_t = jnp.concatenate([got[:, 0], got[:, 2], got[:, 3]], axis=0).reshape(3 * width, tok)
    out_term = jnp.einsum("ct,td->cd", attention_t, cot, preferred_element_type=F32)
    out_term = out_term.astype(BF16).reshape(n_dev, -1, d_slide)
    out_sum = jnp.sum(exchange(out_term, ALL).astype(F32), axis=0)

    embed_grad = (
        cot.astype(F32)
        + jnp.einsum("ct,dc->td", qkv_grad_t, qkv_weight, preferred_element_type=F32)
    ).astype(BF16)

    destination = owner_map[0, :, 0]
    capacity = tile_hidden.shape[1] // n_seq
    onehot = (destination[:, None] == jnp.arange(n_seq, dtype=jnp.int32)[None, :]).astype(F32)
    lower = (
        jnp.arange(tok, dtype=jnp.int32)[:, None] > jnp.arange(tok, dtype=jnp.int32)[None, :]
    ).astype(BF16)
    before = jnp.dot(lower, onehot.astype(BF16), preferred_element_type=F32)
    rank = jnp.sum(before * onehot, axis=1).astype(jnp.int32)
    slot_index = destination * capacity + rank
    selector = (
        jnp.arange(n_seq * capacity, dtype=jnp.int32)[:, None] == slot_index[None, :]
    ).astype(BF16)
    routed = jnp.dot(selector, embed_grad, preferred_element_type=F32).astype(BF16)
    incoming = exchange(routed.reshape(n_seq, capacity, d_slide), SEQ).reshape(-1, d_slide)

    swapped = lax.ppermute(incoming, "co", [(0, 1), (1, 0)])
    term = jnp.einsum("sc,sd->cd", keep, incoming, preferred_element_type=F32)
    term = term + jnp.einsum("sc,sd->cd", other, swapped, preferred_element_type=F32)
    n_zh = lax.axis_size("zh")
    d_tile = embed_weight.shape[0]
    per = d_tile // n_dev
    term = term.astype(BF16).reshape(n_zh, 2, n_seq, per, d_slide).transpose(0, 2, 1, 3, 4)
    term = exchange(term.reshape(n_zh * n_seq, 2, per, d_slide), ("zh",) + SEQ)
    both = exchange(jnp.sum(term.astype(F32), axis=0), "co")
    embed_sum = both[0]
    factor = both[1]

    tile_grad = jnp.einsum("sd,ed->se", incoming, embed_weight, preferred_element_type=F32)
    hidden_grad = jnp.einsum(
        "se,fe->sf", tile_grad.astype(BF16), proj_weight, preferred_element_type=F32
    ).astype(BF16)[None]
    proj_sum = jnp.dot(factor, embed_weight.astype(F32).T, precision=lax.Precision.HIGHEST)
    return (hidden_grad, proj_sum, embed_sum, qkv_sum, out_sum)


def solution(mesh):
    fine = Mesh(mesh.devices.reshape(2, 2, 4, 4, 2), ALL)
    part = P(DP, SEQ, None)
    rows = P(ALL, None)
    return jax.shard_map(
        local,
        mesh=fine,
        in_specs=(part, part, part, P(), P(), P(), P(), part, part, part, P(), P()),
        out_specs=(part, rows, rows, rows, rows),
        check_vma=False,
    )
```

```python
from functools import partial

import jax
import jax.numpy as jnp
from jax import lax
from jax.experimental import pallas as pl
from jax.experimental.pallas import tpu as pltpu
from jax.sharding import Mesh, PartitionSpec as P

F32 = jnp.float32
BF16 = jnp.bfloat16
DP = ("zh", "co")
SEQ = ("y", "x", "zl")
GRP = ("x", "zl")
ALL = DP + SEQ
QB = 256
KC = 512
LOG2E = 1.4426950408889634


def exchange(x, axes):
    return lax.all_to_all(x, axes, 0, 0, tiled=True)


def sent_to_all(x, axes):
    n = lax.axis_size(axes)
    return exchange(jnp.broadcast_to(x[None], (n, *x.shape)), axes)


def blocks_turned(srcs, lane, sub, count):
    outs = []
    for a in range(count):
        out = None
        for b in range(count):
            shift = (b - a) % count * sub
            moved = pltpu.roll(srcs[b], shift, 1) if shift else srcs[b]
            out = moved if out is None else jnp.where(lane == b, moved, out)
        outs.append(out)
    return outs


def attention_kernel(
    par, mine, back, kmat, vmat, kt, vt, code, score, prob, dk, dv, *, hd, tok, nkb, ny, scaling
):
    step = pl.program_id(0)
    length = nkb * tok
    sub = tok // ny
    part = 2 * hd // ny
    off = par[0]
    inv_len, dil, inv_dil = par[1], par[2], par[3]

    def code_of(pos):
        seg = jnp.floor((pos + 0.5) * inv_len)
        res = pos - dil * jnp.floor((pos + 0.5) * inv_dil)
        return seg * 8.0 + res

    @pl.when(step == 0)
    def _():
        for b in range(nkb):
            kb = mine[b, :hd, :]
            vb = mine[b, hd : 2 * hd, :]
            kt[:, b * tok : (b + 1) * tok] = kb
            vt[:, b * tok : (b + 1) * tok] = vb
            kmat[b * tok : (b + 1) * tok, :] = kb.astype(F32).T.astype(BF16)
            vmat[b * tok : (b + 1) * tok, :] = vb.astype(F32).T.astype(BF16)
            pos = lax.broadcasted_iota(jnp.int32, (tok, 128), 0).astype(F32) + float(b * tok)
            code[b * tok : (b + 1) * tok, :] = code_of(pos)
        dk[...] = jnp.zeros_like(dk)
        dv[...] = jnp.zeros_like(dv)

    nb = QB // sub
    lane = lax.broadcasted_iota(jnp.int32, (part, tok), 1) // sub
    tiles = []
    for first in range(0, nb, ny):
        srcs = [mine[step * nb + first + y, 2 * hd :, :].astype(F32) for y in range(ny)]
        tiles.append(jnp.concatenate(blocks_turned(srcs, lane, sub, ny), axis=0))
    qd = jnp.concatenate(tiles, axis=1)
    qt = qd[:hd, :].astype(BF16)
    dot_ = qd[hd:, :]
    qidx = lax.broadcasted_iota(jnp.int32, (8, QB), 1).astype(F32) + (step * QB).astype(F32)
    qpos = qidx + float(tok - sub) * jnp.floor(qidx * (1.0 / sub)) + off
    qcode = code_of(qpos)[0:1, :]

    mx = jnp.full((8, QB), -3e38, F32)
    for c in range(length // KC):
        rows = slice(c * KC, (c + 1) * KC)
        s = jnp.dot(kmat[rows, :], qt, preferred_element_type=F32)
        ck = code[rows, :]
        s = jnp.where(jnp.concatenate([ck] * (QB // 128), axis=1) == qcode, s, -1e30)
        score[rows, :] = s
        mx = jnp.maximum(mx, jnp.max(s.reshape(KC // 8, 8, QB), axis=0))
    top = jnp.max(mx, axis=0, keepdims=True)

    tot = jnp.zeros((8, QB), F32)
    ot = jnp.zeros((hd, QB), F32)
    for c in range(length // KC):
        rows = slice(c * KC, (c + 1) * KC)
        p = jnp.exp2((score[rows, :] - top) * (scaling * LOG2E))
        tot = tot + jnp.sum(p.reshape(KC // 8, 8, QB), axis=0)
        ph = p.astype(BF16)
        prob[rows, :] = ph
        ot = ot + jnp.dot(vt[:, rows], ph, preferred_element_type=F32)
    inv = 1.0 / jnp.sum(tot, axis=0, keepdims=True)
    ot = ot * inv
    dn = dot_ * inv
    dnh = dn.astype(BF16)
    delta = jnp.sum(dnh.astype(F32) * ot, axis=0, keepdims=True)
    dmat = dn.T.astype(BF16)
    qmat = qt.astype(F32).T.astype(BF16)

    dqt = jnp.zeros((hd, QB), F32)
    for c in range(length // KC):
        rows = slice(c * KC, (c + 1) * KC)
        ph = prob[rows, :]
        dp = jnp.dot(vmat[rows, :], dnh, preferred_element_type=F32)
        ds = (ph.astype(F32) * (dp - delta)).astype(BF16)
        dv[rows, :] += jnp.dot(ph, dmat, preferred_element_type=F32)
        dk[rows, :] += jnp.dot(ds, qmat, preferred_element_type=F32)
        dqt = dqt + jnp.dot(kt[:, rows], ds, preferred_element_type=F32)

    both = jnp.concatenate([dqt * scaling, ot], axis=0)
    for first in range(0, nb, ny):
        cols = slice(first * sub, (first + ny) * sub)
        srcs = [both[g * part : (g + 1) * part, cols] for g in range(ny)]
        for y, block in enumerate(blocks_turned(srcs, lane, sub, ny)):
            back[step * nb + first + y, 2 * hd :, :] = block.astype(BF16)

    @pl.when(step == pl.num_programs(0) - 1)
    def _():
        for b in range(nkb):
            rows = slice(b * tok, (b + 1) * tok)
            back[b, :hd, :] = (dk[rows, :].T * scaling).astype(BF16)
            back[b, hd : 2 * hd, :] = dv[rows, :].T.astype(BF16)


def attention_grads(par, mine, hd, ny, scaling):
    nkb, rows, tok = mine.shape
    length = nkb * tok
    steps = length // ny // QB
    whole = pl.BlockSpec((nkb, rows, tok), lambda i: (0, 0, 0))
    return pl.pallas_call(
        partial(attention_kernel, hd=hd, tok=tok, nkb=nkb, ny=ny, scaling=scaling),
        grid=(steps,),
        out_shape=jax.ShapeDtypeStruct((nkb, rows, tok), BF16),
        in_specs=[pl.BlockSpec(memory_space=pltpu.SMEM), whole],
        out_specs=whole,
        scratch_shapes=[
            pltpu.VMEM((length, hd), BF16),
            pltpu.VMEM((length, hd), BF16),
            pltpu.VMEM((hd, length), BF16),
            pltpu.VMEM((hd, length), BF16),
            pltpu.VMEM((length, 128), F32),
            pltpu.VMEM((length, QB), F32),
            pltpu.VMEM((length, QB), BF16),
            pltpu.VMEM((length, hd), F32),
            pltpu.VMEM((length, hd), F32),
        ],
        compiler_params=pltpu.CompilerParams(dimension_semantics=("arbitrary",)),
        cost_estimate=pl.CostEstimate(
            flops=30_000_000_000, bytes_accessed=4_000_000, transcendentals=length * length // ny
        ),
        name="attention_grads",
    )(par, mine)


def pack_kernel(saved, cot, weight, out, *, heads, hd, tok, ny):
    sub = tok // ny
    part = 2 * hd // ny
    width = heads * hd
    grads = lax.dot_general(
        weight[...], cot[...], (((1,), (1,)), ((), ())), preferred_element_type=F32
    )
    grads = grads.astype(BF16).astype(F32)
    saved_t = saved[...].astype(F32).T
    lane = lax.broadcasted_iota(jnp.int32, (part, tok), 1) // sub
    for h in range(heads):
        rows = slice(h * hd, (h + 1) * hd)
        keys = saved_t[width + h * hd : width + (h + 1) * hd, :].astype(BF16)
        values = saved_t[2 * width + h * hd : 2 * width + (h + 1) * hd, :].astype(BF16)
        both = jnp.concatenate([saved_t[rows, :], grads[rows, :]], axis=0)
        srcs = [both[g * part : (g + 1) * part, :] for g in range(ny)]
        for y, block in enumerate(blocks_turned(srcs, lane, sub, ny)):
            out[y * heads + h, :hd, :] = keys
            out[y * heads + h, hd : 2 * hd, :] = values
            out[y * heads + h, 2 * hd :, :] = block.astype(BF16)


def packed(saved, cot, weight, heads, ny):
    tok = saved.shape[0]
    hd = weight.shape[0] // heads
    rows = 2 * hd + 2 * hd // ny
    return pl.pallas_call(
        partial(pack_kernel, heads=heads, hd=hd, tok=tok, ny=ny),
        out_shape=jax.ShapeDtypeStruct((ny * heads, rows, tok), BF16),
        cost_estimate=pl.CostEstimate(
            flops=2 * weight.size * tok, bytes_accessed=2_000_000, transcendentals=0
        ),
        name="packed",
    )(saved, cot, weight)


def unpack_kernel(got, grads, attention, *, heads, hd, tok, ny):
    sub = tok // ny
    part = 2 * hd // ny
    width = heads * hd
    lane = lax.broadcasted_iota(jnp.int32, (part, tok), 1) // sub
    for h in range(heads):
        total = got[h, : 2 * hd, :].astype(F32)
        for y in range(1, ny):
            total = total + got[y * heads + h, : 2 * hd, :].astype(F32)
        total = total.astype(BF16)
        grads[width + h * hd : width + (h + 1) * hd, :] = total[:hd, :]
        grads[2 * width + h * hd : 2 * width + (h + 1) * hd, :] = total[hd:, :]
        srcs = [got[y * heads + h, 2 * hd :, :].astype(F32) for y in range(ny)]
        both = jnp.concatenate(blocks_turned(srcs, lane, sub, ny), axis=0)
        grads[h * hd : (h + 1) * hd, :] = both[:hd, :].astype(BF16)
        attention[h * hd : (h + 1) * hd, :] = both[hd:, :].astype(BF16)


def unpacked(got, heads, hd, ny):
    tok = got.shape[2]
    return pl.pallas_call(
        partial(unpack_kernel, heads=heads, hd=hd, tok=tok, ny=ny),
        out_shape=(
            jax.ShapeDtypeStruct((3 * heads * hd, tok), BF16),
            jax.ShapeDtypeStruct((heads * hd, tok), BF16),
        ),
        cost_estimate=pl.CostEstimate(
            flops=got.size * 100, bytes_accessed=2_000_000, transcendentals=0
        ),
        name="unpacked",
    )(got)


def summed_kernel(keep, other, incoming, swapped, small, out):
    d_slide = incoming.shape[1]
    total = jnp.dot(keep[...], incoming[...], preferred_element_type=F32)
    total = total + jnp.dot(other[...], swapped[...], preferred_element_type=F32)
    out[:, :d_slide] = total.astype(BF16)
    out[:, d_slide:] = small[...]


def summed_terms(keep, other, incoming, swapped, small):
    rows, slots = keep.shape
    d_slide = incoming.shape[1]
    block = 512
    wide = d_slide + small.shape[1]
    whole = pl.BlockSpec((slots, d_slide), lambda i: (0, 0))
    return pl.pallas_call(
        summed_kernel,
        grid=(rows // block,),
        out_shape=jax.ShapeDtypeStruct((rows, wide), BF16),
        in_specs=[
            pl.BlockSpec((block, slots), lambda i: (i, 0)),
            pl.BlockSpec((block, slots), lambda i: (i, 0)),
            whole,
            whole,
            pl.BlockSpec((block, small.shape[1]), lambda i: (i, 0)),
        ],
        out_specs=pl.BlockSpec((block, wide), lambda i: (i, 0)),
        compiler_params=pltpu.CompilerParams(dimension_semantics=("arbitrary",)),
        cost_estimate=pl.CostEstimate(
            flops=4 * rows * slots * d_slide, bytes_accessed=8_000_000, transcendentals=0
        ),
        name="summed_terms",
    )(keep, other, incoming, swapped, small)


def one_hot_rows(source, width, keep=None):
    hit = source[:, None] == jnp.arange(width, dtype=jnp.int32)[None, :]
    if keep is not None:
        hit = hit & keep[:, None]
    return hit.astype(BF16)


def picked_rows(onehot, x):
    return jnp.einsum("rx,tx->rt", onehot, x, preferred_element_type=F32).astype(BF16)


def local(
    tile_embed,
    qkv_saved,
    out_cotangent,
    qkv_weight,
    out_weight,
    seg_length,
    dilation,
    owner_map,
    tile_hidden,
    tile_output,
    embed_weight,
    proj_weight,
):
    heads = seg_length.shape[0]
    width = out_weight.shape[0]
    hd = width // heads
    tok = qkv_saved.shape[1]
    d_slide = tile_embed.shape[2]
    n_seq = lax.axis_size(SEQ)
    n_y = lax.axis_size("y")
    n_dp = lax.axis_size(DP)
    n_dev = n_dp * n_seq
    scaling = hd ** (-0.5)
    cot = out_cotangent[0]
    head = lax.axis_index(GRP)
    core = lax.axis_index("co")

    outgoing = packed(qkv_saved[0], cot, out_weight, heads, n_y)
    outgoing, hidden_rows, output_rows = lax.optimization_barrier(
        (outgoing, tile_hidden[0], tile_output[0])
    )
    mine = exchange(outgoing, SEQ)

    seg = seg_length[head].astype(F32)
    dil = dilation[head].astype(F32)
    off = (lax.axis_index("y") * (tok // n_y)).astype(F32)
    par = jnp.stack([off, 1.0 / seg, dil, 1.0 / dil])
    back = attention_grads(par, mine, hd, n_y, scaling)

    swap = partial(lax.ppermute, axis_name="co", perm=[(0, 1), (1, 0)])
    low = core == 0
    d_tile = embed_weight.shape[0]
    holders = n_dev // 2
    per = d_tile // n_dev
    half = per // 2
    row = jnp.arange(d_tile, dtype=jnp.int32)
    holder = row // (2 * per)
    to_core = row // per % 2
    owner = (holder // n_seq * 2 + to_core) * n_seq + holder % n_seq
    second = row // half % 2 == 1
    spot = row % half
    tile_rows = one_hot_rows(owner * per + row % per, d_tile)
    keep = picked_rows(tile_rows, jnp.where(low, output_rows, hidden_rows))
    other = swap(picked_rows(tile_rows, jnp.where(low, hidden_rows, output_rows)))
    embed_rows = tile_embed[0]
    embed_pair = jnp.concatenate([embed_rows, swap(embed_rows)], axis=0)
    cot_pair = jnp.concatenate([cot, swap(cot)], axis=0)
    first_rows = picked_rows(one_hot_rows(owner * half + spot, d_slide, ~second), embed_pair)
    second_rows = picked_rows(one_hot_rows(owner * half + spot, d_slide, second), embed_pair)
    back, first_rows, second_rows, cot_pair = lax.optimization_barrier(
        (back, first_rows, second_rows, cot_pair)
    )
    got, keep, other = lax.optimization_barrier((exchange(back, SEQ), keep, other))
    qkv_grad_t, attention_t = unpacked(got, heads, hd, n_y)
    query_key, value_t = qkv_grad_t[: 2 * width], qkv_grad_t[2 * width :]
    embed_grad = (
        cot.astype(F32)
        + jnp.einsum("ct,dc->td", qkv_grad_t, qkv_weight, preferred_element_type=F32)
    ).astype(BF16)

    destination = owner_map[0, :, 0]
    capacity = tile_hidden.shape[1] // n_seq
    onehot = (destination[:, None] == jnp.arange(n_seq, dtype=jnp.int32)[None, :]).astype(F32)
    lower = (
        jnp.arange(tok, dtype=jnp.int32)[:, None] > jnp.arange(tok, dtype=jnp.int32)[None, :]
    ).astype(BF16)
    before = jnp.dot(lower, onehot.astype(BF16), preferred_element_type=F32)
    rank = jnp.sum(before * onehot, axis=1).astype(jnp.int32)
    slot_index = destination * capacity + rank
    selector = (
        jnp.arange(n_seq * capacity, dtype=jnp.int32)[:, None] == slot_index[None, :]
    ).astype(BF16)
    routed = jnp.dot(selector, embed_grad, preferred_element_type=F32).astype(BF16)
    value_att = jnp.concatenate([value_t, attention_t], axis=0)
    routed, query_key, value_att = lax.optimization_barrier((routed, query_key, value_att))
    incoming = exchange(routed.reshape(n_seq, capacity, d_slide), SEQ).reshape(-1, d_slide)
    grads = jnp.where(low, query_key, value_att)
    grads = jnp.concatenate([grads, swap(jnp.where(low, value_att, query_key))], axis=1)
    grads = grads.reshape(2, width, 2 * tok)
    o_half = half // 2
    att_row = owner * o_half + spot % o_half
    att_low = jnp.einsum(
        "ra,at->rt",
        one_hot_rows(att_row, width, second & (spot < o_half)),
        grads[1],
        preferred_element_type=F32,
    ).astype(BF16)
    att_high = jnp.einsum(
        "ra,at->rt",
        one_hot_rows(att_row, width, second & (spot >= o_half)),
        grads[1],
        preferred_element_type=F32,
    ).astype(BF16)
    left_side = jnp.concatenate(
        [first_rows, jnp.where(low, second_rows, att_low), jnp.where(low, 0, att_high)], axis=1
    )
    flat = grads.transpose(0, 2, 1)
    right_side = jnp.concatenate(
        [flat[0], jnp.where(low, flat[1], cot_pair[:, :width]), cot_pair[:, width:]], axis=0
    )
    small = jnp.dot(left_side, right_side, preferred_element_type=F32).astype(BF16)
    incoming, small = lax.optimization_barrier((incoming, small))

    term = summed_terms(keep, other, incoming, swap(incoming), small)
    term = term.reshape(holders, -1, term.shape[1])
    held = jnp.sum(exchange(term, ("zh",) + SEQ).astype(F32), axis=0)
    tile_grad = jnp.einsum("sd,ed->se", incoming, embed_weight, preferred_element_type=F32)
    hidden_grad = jnp.einsum(
        "se,fe->sf", tile_grad.astype(BF16), proj_weight, preferred_element_type=F32
    ).astype(BF16)[None]
    held, hidden_grad = lax.optimization_barrier((held, hidden_grad))
    mine_held = jnp.where(low, held[:per], held[per:])
    pair_held = swap(jnp.where(low, held[per:], held[:per]))
    from_low = jnp.where(low, mine_held, pair_held)
    from_high = jnp.where(low, pair_held, mine_held)
    embed_sum = from_low[:, :d_slide]
    factor = from_high[:, :d_slide]
    q_k, v_o = from_low[:, d_slide:], from_high[:, d_slide:]
    qkv_sum = jnp.concatenate([q_k[:half], q_k[half:], v_o[:half]], axis=1)
    out_sum = jnp.concatenate([v_o[half : half + o_half], v_o[half + o_half :]], axis=1)

    proj_sum = jnp.dot(factor, embed_weight.astype(F32).T, precision=lax.Precision.HIGHEST)
    return (hidden_grad, proj_sum, embed_sum, qkv_sum, out_sum)


def solution(mesh):
    fine = Mesh(mesh.devices.reshape(2, 2, 4, 4, 2), ALL)
    part = P(DP, SEQ, None)
    rows = P(ALL, None)
    return jax.shard_map(
        local,
        mesh=fine,
        in_specs=(part, part, part, P(), P(), P(), P(), part, part, part, P(), P()),
        out_specs=(part, rows, rows, rows, rows),
        check_vma=False,
    )
```

```python
from functools import partial

import jax
import jax.numpy as jnp
from jax import lax
from jax.experimental import pallas as pl
from jax.experimental.pallas import tpu as pltpu
from jax.sharding import Mesh, PartitionSpec as P

F32 = jnp.float32
BF16 = jnp.bfloat16
DP = ("zh", "co")
SEQ = ("y", "x", "zl")
GRP = ("x", "zl")
ALL = DP + SEQ
KC = 256
LOG2E = 1.4426950408889634


def near(x):
    return pltpu.with_memory_space_constraint(x, pltpu.VMEM)


def exchange(x, axes):
    return lax.all_to_all(x, axes, 0, 0, tiled=True)


def sent_to_all(x, axes):
    n = lax.axis_size(axes)
    return exchange(jnp.broadcast_to(x[None], (n, *x.shape)), axes)


def blocks_turned(srcs, lane, sub, count):
    outs = []
    for a in range(count):
        out = None
        for b in range(count):
            shift = (b - a) % count * sub
            moved = pltpu.roll(srcs[b], shift, 1) if shift else srcs[b]
            out = moved if out is None else jnp.where(lane == b, moved, out)
        outs.append(out)
    return outs


def attention_kernel(
    par, mine, back, kmat, vmat, kt, vt, code, score, prob, dk, dv, *, hd, tok, nkb, ny, scaling
):
    length = nkb * tok
    qb = length // ny
    sub = tok // ny
    part = 2 * hd // ny
    off = par[0]
    inv_len, dil, inv_dil = par[1], par[2], par[3]

    def code_of(pos):
        seg = jnp.floor((pos + 0.5) * inv_len)
        res = pos - dil * jnp.floor((pos + 0.5) * inv_dil)
        return seg * 8.0 + res

    for b in range(nkb):
        kb = mine[b, :hd, :]
        vb = mine[b, hd : 2 * hd, :]
        kt[:, b * tok : (b + 1) * tok] = kb
        vt[:, b * tok : (b + 1) * tok] = vb
        kmat[b * tok : (b + 1) * tok, :] = kb.astype(F32).T.astype(BF16)
        vmat[b * tok : (b + 1) * tok, :] = vb.astype(F32).T.astype(BF16)
        pos = lax.broadcasted_iota(jnp.int32, (tok, 128), 0).astype(F32) + float(b * tok)
        code[b * tok : (b + 1) * tok, :] = code_of(pos)

    nb = qb // sub
    lane = lax.broadcasted_iota(jnp.int32, (part, tok), 1) // sub
    tiles = []
    for first in range(0, nb, ny):
        srcs = [mine[first + y, 2 * hd :, :].astype(F32) for y in range(ny)]
        tiles.append(jnp.concatenate(blocks_turned(srcs, lane, sub, ny), axis=0))
    qd = jnp.concatenate(tiles, axis=1)
    qt = qd[:hd, :].astype(BF16)
    dot_ = qd[hd:, :]
    qidx = lax.broadcasted_iota(jnp.int32, (8, qb), 1).astype(F32)
    qpos = qidx + float(tok - sub) * jnp.floor(qidx * (1.0 / sub)) + off
    qcode = code_of(qpos)[0:1, :]

    mx = jnp.full((8, qb), -3e38, F32)
    for c in range(length // KC):
        rows = slice(c * KC, (c + 1) * KC)
        s = jnp.dot(kmat[rows, :], qt, preferred_element_type=F32)
        ck = code[rows, :]
        s = jnp.where(jnp.concatenate([ck] * (qb // 128), axis=1) == qcode, s, -1e30)
        score[rows, :] = s
        mx = jnp.maximum(mx, jnp.max(s.reshape(KC // 8, 8, qb), axis=0))
    top = jnp.max(mx, axis=0, keepdims=True)

    tot = jnp.zeros((8, qb), F32)
    ot = jnp.zeros((hd, qb), F32)
    for c in range(length // KC):
        rows = slice(c * KC, (c + 1) * KC)
        p = jnp.exp2((score[rows, :] - top) * (scaling * LOG2E))
        tot = tot + jnp.sum(p.reshape(KC // 8, 8, qb), axis=0)
        ph = p.astype(BF16)
        prob[rows, :] = ph
        ot = ot + jnp.dot(vt[:, rows], ph, preferred_element_type=F32)
    inv = 1.0 / jnp.sum(tot, axis=0, keepdims=True)
    ot = ot * inv
    dn = dot_ * inv
    dnh = dn.astype(BF16)
    delta = jnp.sum(dnh.astype(F32) * ot, axis=0, keepdims=True)
    dmat = dn.T.astype(BF16)
    qmat = qt.astype(F32).T.astype(BF16)

    dqt = jnp.zeros((hd, qb), F32)
    for c in range(length // KC):
        rows = slice(c * KC, (c + 1) * KC)
        ph = prob[rows, :]
        dp = jnp.dot(vmat[rows, :], dnh, preferred_element_type=F32)
        ds = (ph.astype(F32) * (dp - delta)).astype(BF16)
        dv[rows, :] = jnp.dot(ph, dmat, preferred_element_type=F32)
        dk[rows, :] = jnp.dot(ds, qmat, preferred_element_type=F32)
        dqt = dqt + jnp.dot(kt[:, rows], ds, preferred_element_type=F32)

    both = jnp.concatenate([dqt * scaling, ot], axis=0)
    for first in range(0, nb, ny):
        cols = slice(first * sub, (first + ny) * sub)
        srcs = [both[g * part : (g + 1) * part, cols] for g in range(ny)]
        for y, block in enumerate(blocks_turned(srcs, lane, sub, ny)):
            back[first + y, 2 * hd :, :] = block.astype(BF16)

    for b in range(nkb):
        rows = slice(b * tok, (b + 1) * tok)
        back[b, :hd, :] = (dk[rows, :].T * scaling).astype(BF16)
        back[b, hd : 2 * hd, :] = dv[rows, :].T.astype(BF16)


def attention_grads(par, mine, hd, ny, scaling):
    nkb, rows, tok = mine.shape
    length = nkb * tok
    qb = length // ny
    whole = pl.BlockSpec(memory_space=pltpu.VMEM)
    return pl.pallas_call(
        partial(attention_kernel, hd=hd, tok=tok, nkb=nkb, ny=ny, scaling=scaling),
        out_shape=pltpu.VMEM((nkb, rows, tok), BF16),
        in_specs=[pl.BlockSpec(memory_space=pltpu.SMEM), whole],
        out_specs=whole,
        scratch_shapes=[
            pltpu.VMEM((length, hd), BF16),
            pltpu.VMEM((length, hd), BF16),
            pltpu.VMEM((hd, length), BF16),
            pltpu.VMEM((hd, length), BF16),
            pltpu.VMEM((length, 128), F32),
            pltpu.VMEM((length, qb), F32),
            pltpu.VMEM((length, qb), BF16),
            pltpu.VMEM((length, hd), F32),
            pltpu.VMEM((length, hd), F32),
        ],
        cost_estimate=pl.CostEstimate(
            flops=30_000_000_000, bytes_accessed=4_000_000, transcendentals=length * length // ny
        ),
        name="attention_grads",
    )(par, near(mine))


def pack_kernel(saved, cot, weight, out, *, heads, hd, tok, ny):
    sub = tok // ny
    part = 2 * hd // ny
    width = heads * hd
    grads = lax.dot_general(
        weight[...], cot[...], (((1,), (1,)), ((), ())), preferred_element_type=F32
    )
    grads = grads.astype(BF16).astype(F32)
    saved_t = saved[...].astype(F32).T
    lane = lax.broadcasted_iota(jnp.int32, (part, tok), 1) // sub
    for h in range(heads):
        rows = slice(h * hd, (h + 1) * hd)
        keys = saved_t[width + h * hd : width + (h + 1) * hd, :].astype(BF16)
        values = saved_t[2 * width + h * hd : 2 * width + (h + 1) * hd, :].astype(BF16)
        both = jnp.concatenate([saved_t[rows, :], grads[rows, :]], axis=0)
        srcs = [both[g * part : (g + 1) * part, :] for g in range(ny)]
        for y, block in enumerate(blocks_turned(srcs, lane, sub, ny)):
            out[y * heads + h, :hd, :] = keys
            out[y * heads + h, hd : 2 * hd, :] = values
            out[y * heads + h, 2 * hd :, :] = block.astype(BF16)


def packed(saved, cot, weight, heads, ny):
    tok = saved.shape[0]
    hd = weight.shape[0] // heads
    rows = 2 * hd + 2 * hd // ny
    return pl.pallas_call(
        partial(pack_kernel, heads=heads, hd=hd, tok=tok, ny=ny),
        out_shape=jax.ShapeDtypeStruct((ny * heads, rows, tok), BF16),
        cost_estimate=pl.CostEstimate(
            flops=2 * weight.size * tok, bytes_accessed=2_000_000, transcendentals=0
        ),
        in_specs=[pl.BlockSpec(memory_space=pltpu.VMEM)] * 3,
        out_specs=pl.BlockSpec(memory_space=pltpu.VMEM),
        name="packed",
    )(saved, cot, weight)


def token_kernel(core, got, cot_t, weight, selector, routed, own, send, grads, *, heads, hd, ny):
    tok = got.shape[2]
    sub = tok // ny
    part = 2 * hd // ny
    width = heads * hd
    lane = lax.broadcasted_iota(jnp.int32, (part, tok), 1) // sub
    for h in range(heads):
        total = got[h, : 2 * hd, :].astype(F32)
        for y in range(1, ny):
            total = total + got[y * heads + h, : 2 * hd, :].astype(F32)
        total = total.astype(BF16)
        srcs = [got[y * heads + h, 2 * hd :, :].astype(F32) for y in range(ny)]
        both = jnp.concatenate(blocks_turned(srcs, lane, sub, ny), axis=0).astype(BF16)
        rows = [slice(i * width + h * hd, i * width + (h + 1) * hd) for i in range(4)]
        grads[rows[0], :] = both[:hd, :]
        grads[rows[1], :] = total[:hd, :]
        grads[rows[2], :] = total[hd:, :]
        grads[rows[3], :] = both[hd:, :]
    embed_t = jnp.dot(weight[...], grads[: 3 * width, :], preferred_element_type=F32)
    embed_t = (cot_t[...].astype(F32) + embed_t).astype(BF16)
    routed[...] = lax.dot_general(
        selector[...], embed_t, (((1,), (1,)), ((), ())), preferred_element_type=F32
    ).astype(BF16)

    @pl.when(core[0] == 0)
    def _():
        own[...] = grads[: 2 * width, :]
        send[...] = grads[2 * width :, :]

    @pl.when(core[0] != 0)
    def _():
        own[...] = grads[2 * width :, :]
        send[...] = grads[: 2 * width, :]


def token_grads(core, got, cot_t, weight, selector, heads, hd, ny):
    d_slide, tok = cot_t.shape
    vmem = pl.BlockSpec(memory_space=pltpu.VMEM)
    return pl.pallas_call(
        partial(token_kernel, heads=heads, hd=hd, ny=ny),
        out_shape=(
            jax.ShapeDtypeStruct((selector.shape[0], d_slide), BF16),
            jax.ShapeDtypeStruct((2 * heads * hd, tok), BF16),
            jax.ShapeDtypeStruct((2 * heads * hd, tok), BF16),
        ),
        in_specs=[pl.BlockSpec(memory_space=pltpu.SMEM)] + [vmem] * 4,
        out_specs=(vmem, vmem, vmem),
        scratch_shapes=[pltpu.VMEM((4 * heads * hd, tok), BF16)],
        cost_estimate=pl.CostEstimate(
            flops=2 * weight.size * tok, bytes_accessed=4_000_000, transcendentals=0
        ),
        name="token_grads",
    )(core, near(got), near(cot_t), near(weight), near(selector))


def final_kernel(core, mine, pair, weight_t, proj, embed, qkv, out, *, half):
    d_slide = weight_t.shape[0]
    o_half = half // 2
    low = core[0] == 0
    a, b = mine[...], pair[...]
    from_low = jnp.where(low, a, b)
    from_high = jnp.where(low, b, a)
    embed[...] = from_low[:, :d_slide]
    wide = (from_low.shape[1] - d_slide)
    qkv[:, :wide] = from_low[:half, d_slide:]
    qkv[:, wide : 2 * wide] = from_low[half:, d_slide:]
    qkv[:, 2 * wide :] = from_high[:half, d_slide:]
    out[:, :wide] = from_high[half : half + o_half, d_slide:]
    out[:, wide:] = from_high[half + o_half :, d_slide:]
    factor = from_high[:, :d_slide]
    first = factor.astype(BF16)
    rest = factor - first.astype(F32)
    second = rest.astype(BF16)
    third = (rest - second.astype(F32)).astype(BF16)
    total = jnp.dot(first, weight_t[...], preferred_element_type=F32)
    total = total + jnp.dot(second, weight_t[...], preferred_element_type=F32)
    proj[...] = total + jnp.dot(third, weight_t[...], preferred_element_type=F32)


def final_outputs(core, mine, pair, weight_t):
    per, wide = mine.shape
    d_slide, d_tile = weight_t.shape
    half = per // 2
    vmem = pl.BlockSpec(memory_space=pltpu.VMEM)
    return pl.pallas_call(
        partial(final_kernel, half=half),
        out_shape=(
            jax.ShapeDtypeStruct((per, d_tile), F32),
            jax.ShapeDtypeStruct((per, d_slide), F32),
            jax.ShapeDtypeStruct((half, 3 * (wide - d_slide)), F32),
            jax.ShapeDtypeStruct((half // 2, 2 * (wide - d_slide)), F32),
        ),
        in_specs=[pl.BlockSpec(memory_space=pltpu.SMEM)] + [vmem] * 3,
        out_specs=(vmem, vmem, vmem, vmem),
        cost_estimate=pl.CostEstimate(
            flops=6 * per * weight_t.size, bytes_accessed=3_000_000, transcendentals=0
        ),
        name="final_outputs",
    )(core, near(mine), near(pair), near(weight_t))


def summed_kernel(rows, incoming, swapped, small, out, both):
    slots, d_slide = incoming.shape

    @pl.when(pl.program_id(0) == 0)
    def _():
        both[:slots, :] = incoming[...]
        both[slots:, :] = swapped[...]

    out[:, :d_slide] = jnp.dot(rows[...], both[...], preferred_element_type=F32).astype(BF16)
    out[:, d_slide:] = small[...]


def summed_terms(rows, incoming, swapped, small):
    count, depth = rows.shape
    slots, d_slide = incoming.shape
    block = 512
    wide = d_slide + small.shape[1]
    vmem = pl.BlockSpec(memory_space=pltpu.VMEM)
    return pl.pallas_call(
        summed_kernel,
        grid=(count // block,),
        out_shape=jax.ShapeDtypeStruct((count, wide), BF16),
        in_specs=[
            pl.BlockSpec((block, depth), lambda i: (i, 0)),
            vmem,
            vmem,
            pl.BlockSpec((block, small.shape[1]), lambda i: (i, 0)),
        ],
        out_specs=pl.BlockSpec((block, wide), lambda i: (i, 0)),
        scratch_shapes=[pltpu.VMEM((depth, d_slide), BF16)],
        compiler_params=pltpu.CompilerParams(dimension_semantics=("arbitrary",)),
        cost_estimate=pl.CostEstimate(
            flops=2 * count * depth * d_slide, bytes_accessed=8_000_000, transcendentals=0
        ),
        name="summed_terms",
    )(rows, near(incoming), near(swapped), small)


def one_hot_rows(source, width, keep=None):
    hit = source[:, None] == jnp.arange(width, dtype=jnp.int32)[None, :]
    if keep is not None:
        hit = hit & keep[:, None]
    return hit.astype(BF16)


def picked_rows(onehot, x):
    return jnp.einsum("rx,tx->rt", onehot, x, preferred_element_type=F32).astype(BF16)


def local(
    tile_embed,
    qkv_saved,
    out_cotangent,
    qkv_weight,
    out_weight,
    seg_length,
    dilation,
    owner_map,
    tile_hidden,
    tile_output,
    embed_weight,
    proj_weight,
):
    heads = seg_length.shape[0]
    width = out_weight.shape[0]
    hd = width // heads
    tok = qkv_saved.shape[1]
    d_slide = tile_embed.shape[2]
    n_seq = lax.axis_size(SEQ)
    n_y = lax.axis_size("y")
    n_dp = lax.axis_size(DP)
    n_dev = n_dp * n_seq
    scaling = hd ** (-0.5)
    cot = out_cotangent[0]
    head = lax.axis_index(GRP)
    core = lax.axis_index("co")

    destination = owner_map[0, :, 0]
    capacity = tile_hidden.shape[1] // n_seq
    onehot = (destination[:, None] == jnp.arange(n_seq, dtype=jnp.int32)[None, :]).astype(F32)
    lower = (
        jnp.arange(tok, dtype=jnp.int32)[:, None] > jnp.arange(tok, dtype=jnp.int32)[None, :]
    ).astype(BF16)
    before = jnp.dot(lower, onehot.astype(BF16), preferred_element_type=F32)
    rank = jnp.sum(before * onehot, axis=1).astype(jnp.int32)
    slot_index = destination * capacity + rank
    selector = (
        jnp.arange(n_seq * capacity, dtype=jnp.int32)[:, None] == slot_index[None, :]
    ).astype(BF16)
    core_of = core.astype(jnp.int32).reshape(1)
    outgoing = packed(qkv_saved[0], cot, out_weight, heads, n_y)
    outgoing, hidden_rows, output_rows, cot_later = lax.optimization_barrier(
        (outgoing, tile_hidden[0], tile_output[0], cot)
    )
    cot_t = cot_later.T
    mine = exchange(outgoing, SEQ)

    seg = seg_length[head].astype(F32)
    dil = dilation[head].astype(F32)
    off = (lax.axis_index("y") * (tok // n_y)).astype(F32)
    par = jnp.stack([off, 1.0 / seg, dil, 1.0 / dil])
    back = attention_grads(par, mine, hd, n_y, scaling)

    swap = partial(lax.ppermute, axis_name="co", perm=[(0, 1), (1, 0)])
    low = core == 0
    d_tile = embed_weight.shape[0]
    holders = n_dev // 2
    per = d_tile // n_dev
    half = per // 2
    row = jnp.arange(d_tile, dtype=jnp.int32)
    holder = row // (2 * per)
    to_core = row // per % 2
    owner = (holder // n_seq * 2 + to_core) * n_seq + holder % n_seq
    second = row // half % 2 == 1
    spot = row % half
    tile_spots = one_hot_rows(owner * per + row % per, d_tile)
    keep = picked_rows(tile_spots, jnp.where(low, output_rows, hidden_rows))
    other = swap(picked_rows(tile_spots, jnp.where(low, hidden_rows, output_rows)))
    embed_rows = tile_embed[0]
    embed_pair = jnp.concatenate([embed_rows, swap(embed_rows)], axis=0)
    cot_pair = jnp.concatenate([cot, swap(cot)], axis=0)
    first_rows = picked_rows(one_hot_rows(owner * half + spot, d_slide, ~second), embed_pair)
    second_rows = picked_rows(one_hot_rows(owner * half + spot, d_slide, second), embed_pair)
    back, first_rows, second_rows, cot_pair, cot_t, selector = lax.optimization_barrier(
        (back, first_rows, second_rows, cot_pair, cot_t, selector)
    )
    tile_rows = jnp.concatenate([keep, other], axis=1)
    got, tile_rows = lax.optimization_barrier((exchange(back, SEQ), tile_rows))
    routed, own, send = token_grads(core_of, got, cot_t, qkv_weight, selector, heads, hd, n_y)
    incoming = exchange(routed.reshape(n_seq, capacity, d_slide), SEQ).reshape(-1, d_slide)
    grads = jnp.concatenate([own, swap(send)], axis=1)
    grads = grads.reshape(2, width, 2 * tok)
    o_half = half // 2
    att_row = owner * o_half + spot % o_half
    att_low = jnp.einsum(
        "ra,at->rt",
        one_hot_rows(att_row, width, second & (spot < o_half)),
        grads[1],
        preferred_element_type=F32,
    ).astype(BF16)
    att_high = jnp.einsum(
        "ra,at->rt",
        one_hot_rows(att_row, width, second & (spot >= o_half)),
        grads[1],
        preferred_element_type=F32,
    ).astype(BF16)
    left_side = jnp.concatenate(
        [first_rows, jnp.where(low, second_rows, att_low), jnp.where(low, 0, att_high)], axis=1
    )
    flat = grads.transpose(0, 2, 1)
    right_side = jnp.concatenate(
        [flat[0], jnp.where(low, flat[1], cot_pair[:, :width]), cot_pair[:, width:]], axis=0
    )
    small = jnp.dot(left_side, right_side, preferred_element_type=F32).astype(BF16)
    incoming, small = lax.optimization_barrier((incoming, small))

    term = summed_terms(tile_rows, incoming, swap(incoming), small)
    term = term.reshape(holders, -1, term.shape[1])
    held = jnp.sum(exchange(term, ("zh",) + SEQ).astype(F32), axis=0)
    tile_grad = jnp.einsum("sd,ed->se", incoming, embed_weight, preferred_element_type=F32)
    hidden_grad = jnp.einsum(
        "se,fe->sf", tile_grad.astype(BF16), proj_weight, preferred_element_type=F32
    ).astype(BF16)[None]
    held, hidden_grad, weight_t = lax.optimization_barrier((held, hidden_grad, embed_weight.T))
    mine_held = jnp.where(low, held[:per], held[per:])
    pair_held = swap(jnp.where(low, held[per:], held[:per]))
    proj_sum, embed_sum, qkv_sum, out_sum = final_outputs(core_of, mine_held, pair_held, weight_t)
    return (hidden_grad, proj_sum, embed_sum, qkv_sum, out_sum)


def solution(mesh):
    fine = Mesh(mesh.devices.reshape(2, 2, 4, 4, 2), ALL)
    part = P(DP, SEQ, None)
    rows = P(ALL, None)
    return jax.shard_map(
        local,
        mesh=fine,
        in_specs=(part, part, part, P(), P(), P(), P(), part, part, part, P(), P()),
        out_specs=(part, rows, rows, rows, rows),
        check_vma=False,
    )
```

```python
from functools import partial

import jax
import jax.numpy as jnp
from jax import lax
from jax.experimental import pallas as pl
from jax.experimental.pallas import tpu as pltpu
from jax.sharding import Mesh, PartitionSpec as P

F32 = jnp.float32
BF16 = jnp.bfloat16
DP = ("zh", "co")
SEQ = ("y", "x", "zl")
GRP = ("x", "zl")
ALL = DP + SEQ
KC = 256
LOG2E = 1.4426950408889634


def near(x):
    return pltpu.with_memory_space_constraint(x, pltpu.VMEM)


def exchange(x, axes):
    return lax.all_to_all(x, axes, 0, 0, tiled=True)


def sent_to_all(x, axes):
    n = lax.axis_size(axes)
    return exchange(jnp.broadcast_to(x[None], (n, *x.shape)), axes)


def blocks_turned(srcs, lane, sub, count):
    outs = []
    for a in range(count):
        out = None
        for b in range(count):
            shift = (b - a) % count * sub
            moved = pltpu.roll(srcs[b], shift, 1) if shift else srcs[b]
            out = moved if out is None else jnp.where(lane == b, moved, out)
        outs.append(out)
    return outs


def attention_kernel(
    par, mine, back, kmat, vmat, kt, vt, code, score, prob, dk, dv, *, hd, tok, nkb, ny, scaling
):
    length = nkb * tok
    qb = length // ny
    sub = tok // ny
    part = 2 * hd // ny
    off = par[0]
    inv_len, dil, inv_dil = par[1], par[2], par[3]

    def code_of(pos):
        seg = jnp.floor((pos + 0.5) * inv_len)
        res = pos - dil * jnp.floor((pos + 0.5) * inv_dil)
        return seg * 8.0 + res

    for b in range(nkb):
        kb = mine[b, :hd, :]
        vb = mine[b, hd : 2 * hd, :]
        kt[:, b * tok : (b + 1) * tok] = kb
        vt[:, b * tok : (b + 1) * tok] = vb
        kmat[b * tok : (b + 1) * tok, :] = kb.astype(F32).T.astype(BF16)
        vmat[b * tok : (b + 1) * tok, :] = vb.astype(F32).T.astype(BF16)
        pos = lax.broadcasted_iota(jnp.int32, (tok, 128), 0).astype(F32) + float(b * tok)
        code[b * tok : (b + 1) * tok, :] = code_of(pos)

    nb = qb // sub
    lane = lax.broadcasted_iota(jnp.int32, (part, tok), 1) // sub
    tiles = []
    for first in range(0, nb, ny):
        srcs = [mine[first + y, 2 * hd :, :].astype(F32) for y in range(ny)]
        tiles.append(jnp.concatenate(blocks_turned(srcs, lane, sub, ny), axis=0))
    qd = jnp.concatenate(tiles, axis=1)
    qt = qd[:hd, :].astype(BF16)
    dot_ = qd[hd:, :]
    qidx = lax.broadcasted_iota(jnp.int32, (8, qb), 1).astype(F32)
    qpos = qidx + float(tok - sub) * jnp.floor(qidx * (1.0 / sub)) + off
    qcode = code_of(qpos)[0:1, :]

    mx = jnp.full((8, qb), -3e38, F32)
    for c in range(length // KC):
        rows = slice(c * KC, (c + 1) * KC)
        s = jnp.dot(kmat[rows, :], qt, preferred_element_type=F32)
        ck = code[rows, :]
        s = jnp.where(jnp.concatenate([ck] * (qb // 128), axis=1) == qcode, s, -1e30)
        score[rows, :] = s
        mx = jnp.maximum(mx, jnp.max(s.reshape(KC // 8, 8, qb), axis=0))
    top = jnp.max(mx, axis=0, keepdims=True)

    tot = jnp.zeros((8, qb), F32)
    ot = jnp.zeros((hd, qb), F32)
    for c in range(length // KC):
        rows = slice(c * KC, (c + 1) * KC)
        p = jnp.exp2((score[rows, :] - top) * (scaling * LOG2E))
        tot = tot + jnp.sum(p.reshape(KC // 8, 8, qb), axis=0)
        ph = p.astype(BF16)
        prob[rows, :] = ph
        ot = ot + jnp.dot(vt[:, rows], ph, preferred_element_type=F32)
    inv = 1.0 / jnp.sum(tot, axis=0, keepdims=True)
    ot = ot * inv
    dn = dot_ * inv
    dnh = dn.astype(BF16)
    delta = jnp.sum(dnh.astype(F32) * ot, axis=0, keepdims=True)
    dmat = dn.T.astype(BF16)
    qmat = qt.astype(F32).T.astype(BF16)

    dqt = jnp.zeros((hd, qb), F32)
    for c in range(length // KC):
        rows = slice(c * KC, (c + 1) * KC)
        ph = prob[rows, :]
        dp = jnp.dot(vmat[rows, :], dnh, preferred_element_type=F32)
        ds = (ph.astype(F32) * (dp - delta)).astype(BF16)
        dv[rows, :] = jnp.dot(ph, dmat, preferred_element_type=F32)
        dk[rows, :] = jnp.dot(ds, qmat, preferred_element_type=F32)
        dqt = dqt + jnp.dot(kt[:, rows], ds, preferred_element_type=F32)

    both = jnp.concatenate([dqt * scaling, ot], axis=0)
    for first in range(0, nb, ny):
        cols = slice(first * sub, (first + ny) * sub)
        srcs = [both[g * part : (g + 1) * part, cols] for g in range(ny)]
        for y, block in enumerate(blocks_turned(srcs, lane, sub, ny)):
            back[first + y, 2 * hd :, :] = block.astype(BF16)

    for b in range(nkb):
        rows = slice(b * tok, (b + 1) * tok)
        back[b, :hd, :] = (dk[rows, :].T * scaling).astype(BF16)
        back[b, hd : 2 * hd, :] = dv[rows, :].T.astype(BF16)


def attention_grads(par, mine, hd, ny, scaling):
    nkb, rows, tok = mine.shape
    length = nkb * tok
    qb = length // ny
    whole = pl.BlockSpec(memory_space=pltpu.VMEM)
    return pl.pallas_call(
        partial(attention_kernel, hd=hd, tok=tok, nkb=nkb, ny=ny, scaling=scaling),
        out_shape=pltpu.VMEM((nkb, rows, tok), BF16),
        in_specs=[pl.BlockSpec(memory_space=pltpu.SMEM), whole],
        out_specs=whole,
        scratch_shapes=[
            pltpu.VMEM((length, hd), BF16),
            pltpu.VMEM((length, hd), BF16),
            pltpu.VMEM((hd, length), BF16),
            pltpu.VMEM((hd, length), BF16),
            pltpu.VMEM((length, 128), F32),
            pltpu.VMEM((length, qb), F32),
            pltpu.VMEM((length, qb), BF16),
            pltpu.VMEM((length, hd), F32),
            pltpu.VMEM((length, hd), F32),
        ],
        cost_estimate=pl.CostEstimate(
            flops=30_000_000_000, bytes_accessed=4_000_000, transcendentals=length * length // ny
        ),
        name="attention_grads",
    )(par, near(mine))


def pack_kernel(saved, cot, weight, out, *, heads, hd, tok, ny):
    sub = tok // ny
    part = 2 * hd // ny
    width = heads * hd
    grads = lax.dot_general(
        weight[...], cot[...], (((1,), (1,)), ((), ())), preferred_element_type=F32
    )
    grads = grads.astype(BF16).astype(F32)
    saved_t = saved[...].astype(F32).T
    lane = lax.broadcasted_iota(jnp.int32, (part, tok), 1) // sub
    for h in range(heads):
        rows = slice(h * hd, (h + 1) * hd)
        keys = saved_t[width + h * hd : width + (h + 1) * hd, :].astype(BF16)
        values = saved_t[2 * width + h * hd : 2 * width + (h + 1) * hd, :].astype(BF16)
        both = jnp.concatenate([saved_t[rows, :], grads[rows, :]], axis=0)
        srcs = [both[g * part : (g + 1) * part, :] for g in range(ny)]
        for y, block in enumerate(blocks_turned(srcs, lane, sub, ny)):
            out[y * heads + h, :hd, :] = keys
            out[y * heads + h, hd : 2 * hd, :] = values
            out[y * heads + h, 2 * hd :, :] = block.astype(BF16)


def packed(saved, cot, weight, heads, ny):
    tok = saved.shape[0]
    hd = weight.shape[0] // heads
    rows = 2 * hd + 2 * hd // ny
    return pl.pallas_call(
        partial(pack_kernel, heads=heads, hd=hd, tok=tok, ny=ny),
        out_shape=jax.ShapeDtypeStruct((ny * heads, rows, tok), BF16),
        cost_estimate=pl.CostEstimate(
            flops=2 * weight.size * tok, bytes_accessed=2_000_000, transcendentals=0
        ),
        in_specs=[pl.BlockSpec(memory_space=pltpu.VMEM)] * 3,
        out_specs=pl.BlockSpec(memory_space=pltpu.VMEM),
        name="packed",
    )(saved, cot, weight)


def token_kernel(core, got, cot, weight, selector, routed, own, send, grads, *, heads, hd, ny):
    tok = got.shape[2]
    sub = tok // ny
    part = 2 * hd // ny
    width = heads * hd
    lane = lax.broadcasted_iota(jnp.int32, (part, tok), 1) // sub
    for h in range(heads):
        total = got[h, : 2 * hd, :].astype(F32)
        for y in range(1, ny):
            total = total + got[y * heads + h, : 2 * hd, :].astype(F32)
        total = total.astype(BF16)
        srcs = [got[y * heads + h, 2 * hd :, :].astype(F32) for y in range(ny)]
        both = jnp.concatenate(blocks_turned(srcs, lane, sub, ny), axis=0).astype(BF16)
        rows = [slice(i * width + h * hd, i * width + (h + 1) * hd) for i in range(4)]
        grads[rows[0], :] = both[:hd, :]
        grads[rows[1], :] = total[:hd, :]
        grads[rows[2], :] = total[hd:, :]
        grads[rows[3], :] = both[hd:, :]
    embed_t = jnp.dot(weight[...], grads[: 3 * width, :], preferred_element_type=F32)
    embed_t = (cot[...].astype(F32).T + embed_t).astype(BF16)
    routed[...] = lax.dot_general(
        selector[...], embed_t, (((1,), (1,)), ((), ())), preferred_element_type=F32
    ).astype(BF16)

    @pl.when(core[0] == 0)
    def _():
        own[...] = grads[: 2 * width, :]
        send[...] = grads[2 * width :, :]

    @pl.when(core[0] != 0)
    def _():
        own[...] = grads[2 * width :, :]
        send[...] = grads[: 2 * width, :]


def token_grads(core, got, cot, weight, selector, heads, hd, ny):
    tok, d_slide = cot.shape
    vmem = pl.BlockSpec(memory_space=pltpu.VMEM)
    return pl.pallas_call(
        partial(token_kernel, heads=heads, hd=hd, ny=ny),
        out_shape=(
            jax.ShapeDtypeStruct((selector.shape[0], d_slide), BF16),
            jax.ShapeDtypeStruct((2 * heads * hd, tok), BF16),
            jax.ShapeDtypeStruct((2 * heads * hd, tok), BF16),
        ),
        in_specs=[pl.BlockSpec(memory_space=pltpu.SMEM)] + [vmem] * 4,
        out_specs=(vmem, vmem, vmem),
        scratch_shapes=[pltpu.VMEM((4 * heads * hd, tok), BF16)],
        cost_estimate=pl.CostEstimate(
            flops=2 * weight.size * tok, bytes_accessed=4_000_000, transcendentals=0
        ),
        name="token_grads",
    )(core, near(got), cot, near(weight), near(selector))


def final_kernel(core, mine, pair, weight_t, proj, embed, qkv, out, *, half):
    d_slide = weight_t.shape[0]
    o_half = half // 2
    low = core[0] == 0
    a, b = mine[...], pair[...]
    from_low = jnp.where(low, a, b)
    from_high = jnp.where(low, b, a)
    embed[...] = from_low[:, :d_slide]
    wide = (from_low.shape[1] - d_slide)
    qkv[:, :wide] = from_low[:half, d_slide:]
    qkv[:, wide : 2 * wide] = from_low[half:, d_slide:]
    qkv[:, 2 * wide :] = from_high[:half, d_slide:]
    out[:, :wide] = from_high[half : half + o_half, d_slide:]
    out[:, wide:] = from_high[half + o_half :, d_slide:]
    factor = from_high[:, :d_slide]
    first = factor.astype(BF16)
    rest = factor - first.astype(F32)
    second = rest.astype(BF16)
    third = (rest - second.astype(F32)).astype(BF16)
    total = jnp.dot(first, weight_t[...], preferred_element_type=F32)
    total = total + jnp.dot(second, weight_t[...], preferred_element_type=F32)
    proj[...] = total + jnp.dot(third, weight_t[...], preferred_element_type=F32)


def final_outputs(core, mine, pair, weight_t):
    per, wide = mine.shape
    d_slide, d_tile = weight_t.shape
    half = per // 2
    vmem = pl.BlockSpec(memory_space=pltpu.VMEM)
    return pl.pallas_call(
        partial(final_kernel, half=half),
        out_shape=(
            jax.ShapeDtypeStruct((per, d_tile), F32),
            jax.ShapeDtypeStruct((per, d_slide), F32),
            jax.ShapeDtypeStruct((half, 3 * (wide - d_slide)), F32),
            jax.ShapeDtypeStruct((half // 2, 2 * (wide - d_slide)), F32),
        ),
        in_specs=[pl.BlockSpec(memory_space=pltpu.SMEM)] + [vmem] * 3,
        out_specs=(vmem, vmem, vmem, vmem),
        cost_estimate=pl.CostEstimate(
            flops=6 * per * weight_t.size, bytes_accessed=3_000_000, transcendentals=0
        ),
        name="final_outputs",
    )(core, near(mine), near(pair), near(weight_t))


def summed_kernel(rows, incoming, swapped, small, out, both):
    slots, d_slide = incoming.shape

    @pl.when(pl.program_id(0) == 0)
    def _():
        both[:slots, :] = incoming[...]
        both[slots:, :] = swapped[...]

    out[:, :d_slide] = jnp.dot(rows[...], both[...], preferred_element_type=F32).astype(BF16)
    out[:, d_slide:] = small[...]


def summed_terms(rows, incoming, swapped, small):
    count, depth = rows.shape
    slots, d_slide = incoming.shape
    block = 512
    wide = d_slide + small.shape[1]
    vmem = pl.BlockSpec(memory_space=pltpu.VMEM)
    return pl.pallas_call(
        summed_kernel,
        grid=(count // block,),
        out_shape=jax.ShapeDtypeStruct((count, wide), BF16),
        in_specs=[
            pl.BlockSpec((block, depth), lambda i: (i, 0)),
            vmem,
            vmem,
            pl.BlockSpec((block, small.shape[1]), lambda i: (i, 0)),
        ],
        out_specs=pl.BlockSpec((block, wide), lambda i: (i, 0)),
        scratch_shapes=[pltpu.VMEM((depth, d_slide), BF16)],
        compiler_params=pltpu.CompilerParams(dimension_semantics=("arbitrary",)),
        cost_estimate=pl.CostEstimate(
            flops=2 * count * depth * d_slide, bytes_accessed=8_000_000, transcendentals=0
        ),
        name="summed_terms",
    )(rows, near(incoming), near(swapped), small)


def one_hot_rows(source, width, keep=None):
    hit = source[:, None] == jnp.arange(width, dtype=jnp.int32)[None, :]
    if keep is not None:
        hit = hit & keep[:, None]
    return hit.astype(BF16)


def picked_rows(onehot, x):
    return jnp.einsum("rx,tx->rt", onehot, x, preferred_element_type=F32).astype(BF16)


def local(
    tile_embed,
    qkv_saved,
    out_cotangent,
    qkv_weight,
    out_weight,
    seg_length,
    dilation,
    owner_map,
    tile_hidden,
    tile_output,
    embed_weight,
    proj_weight,
):
    heads = seg_length.shape[0]
    width = out_weight.shape[0]
    hd = width // heads
    tok = qkv_saved.shape[1]
    d_slide = tile_embed.shape[2]
    n_seq = lax.axis_size(SEQ)
    n_y = lax.axis_size("y")
    n_dp = lax.axis_size(DP)
    n_dev = n_dp * n_seq
    scaling = hd ** (-0.5)
    cot = out_cotangent[0]
    head = lax.axis_index(GRP)
    core = lax.axis_index("co")

    destination = owner_map[0, :, 0]
    capacity = tile_hidden.shape[1] // n_seq
    onehot = (destination[:, None] == jnp.arange(n_seq, dtype=jnp.int32)[None, :]).astype(F32)
    lower = (
        jnp.arange(tok, dtype=jnp.int32)[:, None] > jnp.arange(tok, dtype=jnp.int32)[None, :]
    ).astype(BF16)
    before = jnp.dot(lower, onehot.astype(BF16), preferred_element_type=F32)
    rank = jnp.sum(before * onehot, axis=1).astype(jnp.int32)
    slot_index = destination * capacity + rank
    selector = (
        jnp.arange(n_seq * capacity, dtype=jnp.int32)[:, None] == slot_index[None, :]
    ).astype(BF16)
    core_of = core.astype(jnp.int32).reshape(1)
    outgoing = packed(qkv_saved[0], cot, out_weight, heads, n_y)
    outgoing, hidden_rows, output_rows = lax.optimization_barrier(
        (outgoing, tile_hidden[0], tile_output[0])
    )
    mine = exchange(outgoing, SEQ)

    seg = seg_length[head].astype(F32)
    dil = dilation[head].astype(F32)
    off = (lax.axis_index("y") * (tok // n_y)).astype(F32)
    par = jnp.stack([off, 1.0 / seg, dil, 1.0 / dil])
    back = attention_grads(par, mine, hd, n_y, scaling)

    swap = partial(lax.ppermute, axis_name="co", perm=[(0, 1), (1, 0)])
    low = core == 0
    d_tile = embed_weight.shape[0]
    holders = n_dev // 2
    per = d_tile // n_dev
    half = per // 2
    row = jnp.arange(d_tile, dtype=jnp.int32)
    holder = row // (2 * per)
    to_core = row // per % 2
    owner = (holder // n_seq * 2 + to_core) * n_seq + holder % n_seq
    second = row // half % 2 == 1
    spot = row % half
    tile_spots = one_hot_rows(owner * per + row % per, d_tile)
    keep = picked_rows(tile_spots, jnp.where(low, output_rows, hidden_rows))
    other = swap(picked_rows(tile_spots, jnp.where(low, hidden_rows, output_rows)))
    embed_rows = tile_embed[0]
    embed_pair = jnp.concatenate([embed_rows, swap(embed_rows)], axis=0)
    cot_pair = jnp.concatenate([cot, swap(cot)], axis=0)
    first_rows = picked_rows(one_hot_rows(owner * half + spot, d_slide, ~second), embed_pair)
    second_rows = picked_rows(one_hot_rows(owner * half + spot, d_slide, second), embed_pair)
    back, first_rows, second_rows, cot_pair, selector = lax.optimization_barrier(
        (back, first_rows, second_rows, cot_pair, selector)
    )
    tile_rows = jnp.concatenate([keep, other], axis=1)
    got, tile_rows = lax.optimization_barrier((exchange(back, SEQ), tile_rows))
    routed, own, send = token_grads(core_of, got, cot, qkv_weight, selector, heads, hd, n_y)
    incoming = exchange(routed.reshape(n_seq, capacity, d_slide), SEQ).reshape(-1, d_slide)
    grads = jnp.concatenate([own, swap(send)], axis=1)
    grads = grads.reshape(2, width, 2 * tok)
    o_half = half // 2
    att_row = owner * o_half + spot % o_half
    att_low = jnp.einsum(
        "ra,at->rt",
        one_hot_rows(att_row, width, second & (spot < o_half)),
        grads[1],
        preferred_element_type=F32,
    ).astype(BF16)
    att_high = jnp.einsum(
        "ra,at->rt",
        one_hot_rows(att_row, width, second & (spot >= o_half)),
        grads[1],
        preferred_element_type=F32,
    ).astype(BF16)
    left_side = jnp.concatenate(
        [first_rows, jnp.where(low, second_rows, att_low), jnp.where(low, 0, att_high)], axis=1
    )
    flat = grads.transpose(0, 2, 1)
    right_side = jnp.concatenate(
        [flat[0], jnp.where(low, flat[1], cot_pair[:, :width]), cot_pair[:, width:]], axis=0
    )
    small = jnp.dot(left_side, right_side, preferred_element_type=F32).astype(BF16)

    incoming, small = lax.optimization_barrier((incoming, small))
    term = summed_terms(tile_rows, incoming, swap(incoming), small)
    term = term.reshape(holders, -1, term.shape[1])
    held = jnp.sum(exchange(term, ("zh",) + SEQ).astype(F32), axis=0)
    tile_grad = jnp.einsum("sd,ed->se", incoming, embed_weight, preferred_element_type=F32)
    hidden_grad = jnp.einsum(
        "se,fe->sf", tile_grad.astype(BF16), proj_weight, preferred_element_type=F32
    ).astype(BF16)[None]
    held, hidden_grad, weight_t = lax.optimization_barrier((held, hidden_grad, embed_weight.T))
    mine_held = jnp.where(low, held[:per], held[per:])
    pair_held = swap(jnp.where(low, held[per:], held[:per]))
    proj_sum, embed_sum, qkv_sum, out_sum = final_outputs(core_of, mine_held, pair_held, weight_t)
    return (hidden_grad, proj_sum, embed_sum, qkv_sum, out_sum)


def solution(mesh):
    fine = Mesh(mesh.devices.reshape(2, 2, 4, 4, 2), ALL)
    part = P(DP, SEQ, None)
    rows = P(ALL, None)
    return jax.shard_map(
        local,
        mesh=fine,
        in_specs=(part, part, part, P(), P(), P(), P(), part, part, part, P(), P()),
        out_specs=(part, rows, rows, rows, rows),
        check_vma=False,
    )
```
